256 devices in a mesh: dp: 32 (over z, x_lo, core), comp: 8 (over y, x_hi).
Axes of the slice: x: 4 (x_hi: 2, x_lo: 2; x = x_hi * 2 + x_lo), y: 4, z: 8, core: 2. Of those that a mesh axis runs over, the one named last changes fastest.
Arguments:
- points: float32 [262144, 128], P('dp'), may hold values from -8 to 8
- means: float32 [4096, 128], P('comp'), may hold values from -3 to 3
- variances: float32 [4096, 128], P('comp'), may hold values from 0.5 to 4
- log_weights: float32 [4096], P('comp'), may hold values from -2 to 2
Outputs:
- log_lik: float32 [262144], P('dp')
- new_means: float32 [4096, 128], P('comp')
- new_variances: float32 [4096, 128], P('comp')
- new_log_weights: float32 [4096], P('comp')
The draws below stay inside these ranges and needn't reach their ends.
All inputs are finite; a program needn't handle non-finite values.
Results may differ from the reference program's by a relative error of at most 0.0003.
Values sent between devices are 32-bit elements; how exact they have to be, the bound alone decides.
No kernel may reach another device: no remote copies, remote signals or barrier semaphores. Data moves between devices by JAX's collectives and lax.ppermute only.
A program may use at most 128 MiB of HBM per device.

```python
import math
import jax
import jax.numpy as jnp
from jax import lax

K = 4096
D = 128
N_POINTS = 262144


def draw_points(key, part):
    first_key = jax.random.fold_in(jax.random.fold_in(key, 11), 0)
    flag_key, reach_key = jax.random.split(jax.random.fold_in(key, 23))
    far_rows = (jax.random.randint(flag_key, (N_POINTS, 1), 0, 4) == 0).astype(jnp.float32)
    reach = jnp.exp(jax.random.uniform(reach_key, (N_POINTS, 1), jnp.float32, 0.0, 0.5878))
    shift = far_rows * reach * (22.0 / D ** 0.5)
    values = jnp.clip(jax.random.normal(first_key, (N_POINTS, D), jnp.float32), -6.0, 6.0)
    values = jnp.clip(values + shift, -8.0, 8.0)
    return values.astype(jnp.float32)


def levels(key, shape, cuts, low, largest):
    loudness = 1.0
    for position, blocks in cuts:
        draws = jax.random.uniform(jax.random.fold_in(jax.random.fold_in(key, 6), position), (blocks,), jnp.float32, low / len(cuts), largest / len(cuts))
        loudness = loudness * jnp.repeat(jnp.exp(draws), shape[position] // blocks).reshape((-1,) + (1,) * (len(shape) - 1 - position))
    return loudness


def noise(stream_key, shape, spread, most, cuts=(), dtype=jnp.bfloat16):
    result = spread * jax.random.normal(stream_key, shape, jnp.float32)
    if cuts:
        result = result * levels(stream_key, shape, cuts, -0.22, 0.18)
    return jnp.clip(result, -most, most).astype(dtype)


def setup_inputs(seed: int = 0) -> dict:
    arg_keys = jax.random.split(jax.random.key(seed), 5)
    return {
        "points": draw_points(jax.random.fold_in(arg_keys[4], 71), 0),
        "means": noise(arg_keys[1], (K, D), 0.5, 3.0, ((0, 8),), jnp.float32),
        "variances": jnp.clip(jnp.exp(math.log(4.0) - 2.0794415 * jax.random.uniform(arg_keys[2], (K, D), jnp.float32) ** levels(arg_keys[2], (K, D), ((0, 8),), -0.2, 0.2)), 0.5, 4.0),
        "log_weights": jnp.clip(jax.random.uniform(arg_keys[3], (K,), jnp.float32, -2.0, 2.0) * levels(arg_keys[3], (K,), ((0, 8),), -0.4, 0.0), -2.0, 2.0),
    }


LOG_TWO_PI = math.log(2.0 * math.pi)
PRIOR = 1.0


def densities(block, means, variances, log_weights):
    inverse = 1.0 / variances
    scaled = means * inverse
    offset = log_weights - 0.5 * (jnp.sum(means * scaled, axis=1) + jnp.sum(jnp.log(variances), axis=1) + means.shape[1] * LOG_TWO_PI)
    highest = lax.Precision.HIGHEST
    linear = jnp.dot(block, scaled.T, precision=highest, preferred_element_type=jnp.float32)
    square = jnp.dot(block * block, inverse.T, precision=highest, preferred_element_type=jnp.float32)
    return offset[None, :] + linear - 0.5 * square


def update(counts, first, second, means, variances, total_points, total_comps):
    denom = (counts + PRIOR)[:, None]
    fresh_means = (first + PRIOR * means) / denom
    fresh_vars = (second + PRIOR * (variances + means * means)) / denom - fresh_means * fresh_means
    fresh_logw = jnp.log((counts + PRIOR) / (total_points + PRIOR * total_comps))
    return fresh_means, fresh_vars, fresh_logw


def reference(points, means, variances, log_weights):
    rows = math.gcd(N_POINTS, 4096)
    blocks = points.reshape(-1, rows, D)
    highest = lax.Precision.HIGHEST
    contract = (((0,), (0,)), ((), ()))

    def advance(carry, block):
        counts, first, second = carry
        logp = densities(block, means, variances, log_weights)
        top = jnp.max(logp, axis=1)
        total = top + jnp.log(jnp.sum(jnp.exp(logp - top[:, None]), axis=1))
        resp = jnp.exp(logp - total[:, None])
        counts = counts + jnp.sum(resp, axis=0)
        first = first + lax.dot_general(resp, block, contract, precision=highest, preferred_element_type=jnp.float32)
        second = second + lax.dot_general(resp, block * block, contract, precision=highest, preferred_element_type=jnp.float32)
        return (counts, first, second), total

    start = (jnp.zeros((K,), jnp.float32), jnp.zeros((K, D), jnp.float32), jnp.zeros((K, D), jnp.float32))
    (counts, first, second), totals = lax.scan(advance, start, blocks)
    fresh_means, fresh_vars, fresh_logw = update(counts, first, second, means, variances, float(N_POINTS), float(K))
    return totals.reshape(-1), fresh_means, fresh_vars, fresh_logw
```

```python
import functools
import math

import jax
import jax.numpy as jnp
from jax import lax
from jax.experimental import pallas as pl
from jax.experimental.pallas import tpu as pltpu
from jax.sharding import Mesh, PartitionSpec as P

LOG_TWO_PI = math.log(2.0 * math.pi)
LOG2E = math.log2(math.e)
LN2 = math.log(2.0)
PRIOR = 1.0
LIMIT = 10
TILE = 256
GROUPS = 16
PARTS = 2
F32 = jnp.float32
BF16 = jnp.bfloat16

DP = ("z", "xl", "co")
RING = ("xl", "z")
COMP = ("y", "xh")
ROWS = 16
TALL = 40

NT = (((1,), (1,)), ((), ()))


def halves(a):
    high = a.astype(BF16)
    low = (a - high.astype(F32)).astype(BF16)
    return high, low


def point_halves(x):
    xh, xl = halves(x)
    qh, ql = halves(x * x)
    return jnp.concatenate([xh, qh], axis=1), jnp.concatenate([xl, ql], axis=1)


def density_kernel(at_ref, x_hbm, mean_ref, var_ref, logw_ref, e_ref, p_ref, q_ref, m_ref, l_ref, own_ref, wh_ref, wl_ref, off_ref, x_ref, sems):
    step = pl.program_id(0)
    d = x_ref.shape[1]
    steps = sems.shape[0]
    block = x_ref.shape[0] // steps

    def fetch(i):
        some = pl.ds(pl.multiple_of(i * block, block), block)
        return pltpu.make_async_copy(x_hbm.at[some, :], x_ref.at[some, :], sems.at[i])

    @pl.when(step == 0)
    def _():
        for i in range(steps):
            fetch(i).start()

    @pl.when(step == 0)
    def _():
        mean = mean_ref[...]
        var = var_ref[...]
        inverse = 1.0 / var
        scaled = mean * inverse
        size = jnp.sum(mean * scaled + jnp.log(var), axis=1, keepdims=True)
        logw = jnp.swapaxes(jnp.broadcast_to(logw_ref[...], (128, logw_ref.shape[1])), 0, 1)
        off = logw - 0.5 * (size + d * LOG_TWO_PI)
        off = jnp.broadcast_to((off * LOG2E)[:, :1], off_ref.shape)
        off_ref[...] = off
        w = jnp.concatenate([scaled * LOG2E, inverse * (-0.5 * LOG2E)], axis=1)
        wh_ref[...], wl_ref[...] = halves(w)
        begin = pl.multiple_of(at_ref[2], ROWS)
        own_ref[:ROWS, :] = mean_ref[pl.ds(begin, ROWS), :]
        own_ref[ROWS:, :] = var_ref[pl.ds(begin, ROWS), :]

    wh = wh_ref[...]
    wl = wl_ref[...]
    groups, size = GROUPS, wh.shape[0] // GROUPS

    def mul(a, b):
        return lax.dot_general(a, b, NT, preferred_element_type=F32)

    fetch(step).wait()
    for tile in range(0, block, TILE):
        rows = pl.ds(pl.multiple_of(step * block + tile, TILE), TILE)
        index = step * (block // TILE) + tile // TILE
        ph, plo = point_halves(x_ref[rows, :])
        p_ref[rows, :] = ph
        q_ref[rows, :] = plo
        logp = mul(wh, ph) + mul(wl, ph) + mul(wh, plo)
        tops = []
        sums = []
        for g in range(groups):
            at = slice(g * size, (g + 1) * size)
            part = logp[at, :] + off_ref[at, :]
            part = part.reshape(size // 8, 8, TILE)
            top = jnp.max(part, axis=0)
            e = jnp.exp2(part - top[None])
            e_ref[index, at, :] = e.reshape(size, TILE)
            m_ref[8 * g : 8 * g + 8, rows] = top
            tops.append(top)
            sums.append(jnp.sum(e, axis=0))
        top = jnp.max(functools.reduce(jnp.maximum, tops), axis=0, keepdims=True)
        s = sum(a * jnp.exp2(t - top) for a, t in zip(sums, tops))
        local = top + jnp.log2(jnp.sum(s, axis=0, keepdims=True))
        for i in range(l_ref.shape[0]):
            l_ref[i, :, rows] = local


def densities(points, means, variances, log_weights, table, copies, block):
    n, d = points.shape
    k = means.shape[0]
    const = lambda i, at: (0, 0)
    vmem = pl.BlockSpec(memory_space=pltpu.VMEM)
    return pl.pallas_call(
        density_kernel,
        grid_spec=pltpu.PrefetchScalarGridSpec(
            num_scalar_prefetch=1,
            grid=(n // block,),
            in_specs=[
                pl.BlockSpec(memory_space=pltpu.HBM),
                pl.BlockSpec((k, d), const),
                pl.BlockSpec((k, d), const),
                pl.BlockSpec((1, k), const),
            ],
            out_specs=[vmem] * 6,
            scratch_shapes=[
                pltpu.VMEM((k, 2 * d), BF16),
                pltpu.VMEM((k, 2 * d), BF16),
                pltpu.VMEM((k, TILE), F32),
                pltpu.VMEM((n, d), F32),
                pltpu.SemaphoreType.DMA((n // block,)),
            ],
        ),
        out_shape=[
            pltpu.VMEM((n // TILE, k, TILE), F32),
            pltpu.VMEM((n, 2 * d), BF16),
            pltpu.VMEM((n, 2 * d), BF16),
            pltpu.VMEM((8 * GROUPS, n), F32),
            pltpu.VMEM((copies, 1, n), F32),
            pltpu.VMEM((2 * ROWS, d), F32),
        ],
        compiler_params=pltpu.CompilerParams(vmem_limit_bytes=LIMIT << 20),
        cost_estimate=pl.CostEstimate(
            flops=12 * n * k * d, bytes_accessed=4 * n * (k + d), transcendentals=n * k
        ),
        name="density",
    )(
        table,
        in_hbm(points),
        in_hbm(means),
        in_hbm(variances),
        in_hbm(log_weights.reshape(1, k)),
    )


def in_hbm(array):
    return pltpu.with_memory_space_constraint(array, pltpu.HBM)


def in_vmem(*arrays):
    return [pltpu.with_memory_space_constraint(a, pltpu.VMEM) for a in arrays]


def moment_kernel(table_ref, e_ref, p_ref, q_ref, m_ref, sum_ref, *refs, block, first, places):
    if first:
        lik_hbm, total_ref, *refs = refs
        *refs, lik_ref, sem = refs
    else:
        total_ref = sum_ref
    *out_refs, acc_ref, cnt_ref = refs
    step = pl.program_id(0)
    size = e_ref.shape[1] // GROUPS
    pieces, _, d = out_refs[0].shape
    groups = pieces * ROWS // size

    @pl.when(step == 0)
    def _():
        acc_ref[...] = jnp.zeros_like(acc_ref)
        cnt_ref[...] = jnp.zeros_like(cnt_ref)
        if first:
            sums = sum_ref[:, 0, :]
            top = jnp.max(sums, axis=0, keepdims=True)
            total = top + jnp.log2(jnp.sum(jnp.exp2(sums - top), axis=0, keepdims=True))
            total_ref[...] = total
            lik_ref[...] = total * LN2
            pltpu.make_async_copy(lik_ref, lik_hbm, sem).start()

    def mul(a, b):
        return jnp.dot(a, b, preferred_element_type=F32)

    acc = None
    for tile in range(0, block, TILE):
        some = pl.ds(pl.multiple_of(step * block + tile, TILE), TILE)
        index = step * (block // TILE) + tile // TILE
        total = total_ref[:, some]
        parts = []
        for place in places:
            for g in range(groups):
                at = table_ref[place] * groups + g
                rows = pl.ds(pl.multiple_of(at * size, size), size)
                part = e_ref[index, rows, :].reshape(size // 8, 8, TILE)
                tops = m_ref[pl.ds(pl.multiple_of(at * 8, 8), 8), some]
                parts.append((part * jnp.exp2(tops - total)[None]).reshape(size, TILE))
        resp = jnp.concatenate(parts, axis=0)
        part = sum(resp[:, i : i + 128] for i in range(0, TILE, 128))
        count = part if tile == 0 else count + part
        rh, rl = halves(resp)
        ph = p_ref[some, :]
        part = mul(rh, ph) + mul(rl, ph) + mul(rh, q_ref[some, :])
        acc = part if tile == 0 else acc + part
    cnt_ref[...] += count
    acc_ref[...] += acc

    @pl.when(step == pl.num_programs(0) - 1)
    def _():
        if first:
            pltpu.make_async_copy(lik_ref, lik_hbm, sem).wait()
        count = jnp.sum(cnt_ref[...], axis=1, keepdims=True)
        count = jnp.broadcast_to(count, cnt_ref.shape).reshape(-1, pieces, 2, ROWS // 2, d)
        lane = lax.broadcasted_iota(jnp.int32, (pieces, ROWS // 2, d), 2)
        for i, out_ref in enumerate(out_refs):
            at = slice(i * pieces * ROWS, (i + 1) * pieces * ROWS)
            out_ref[:, 0:ROWS, :] = acc_ref[at, :d].reshape(pieces, ROWS, d)
            out_ref[:, ROWS : 2 * ROWS, :] = acc_ref[at, d:].reshape(pieces, ROWS, d)
            out_ref[:, 2 * ROWS :, :] = jnp.where(lane < d // 2, count[i, :, 0], count[i, :, 1])


def moments(table, places, e, p, q, m, sums, block, first):
    k = e.shape[1] // PARTS
    n, d = p.shape[0], p.shape[1] // 2
    pieces = k // ROWS
    rows = k * len(places)
    vmem = pl.BlockSpec(memory_space=pltpu.VMEM)

    def kernel(*refs):
        moment_kernel(*refs, block=block, first=first, places=places)

    out_specs = [vmem for _ in places]
    out_shape = [pltpu.VMEM((pieces, TALL, d), F32) for _ in places]
    scratch = [pltpu.VMEM((rows, 2 * d), F32), pltpu.VMEM((rows, 128), F32)]
    if first:
        out_specs = [pl.BlockSpec(memory_space=pltpu.HBM), vmem, *out_specs]
        out_shape = [pltpu.HBM((1, n), F32), pltpu.VMEM((1, n), F32), *out_shape]
        scratch += [pltpu.VMEM((1, n), F32), pltpu.SemaphoreType.DMA]
    return pl.pallas_call(
        kernel,
        grid_spec=pltpu.PrefetchScalarGridSpec(
            num_scalar_prefetch=1,
            grid=(n // block,),
            in_specs=[vmem] * 5,
            out_specs=out_specs,
            scratch_shapes=scratch,
        ),
        out_shape=out_shape,
        compiler_params=pltpu.CompilerParams(vmem_limit_bytes=LIMIT << 20),
        cost_estimate=pl.CostEstimate(
            flops=12 * n * rows * d, bytes_accessed=4 * n * (rows + d), transcendentals=n
        ),
        name="moment",
    )(table, *in_vmem(e, p, q, m, sums))


def summed(*arrays):
    def kernel(*refs):
        refs[-1][...] = functools.reduce(lambda a, b: a + b, [r[...] for r in refs[:-1]])

    return pl.pallas_call(
        kernel,
        out_shape=pltpu.VMEM(arrays[0].shape, F32),
        compiler_params=pltpu.CompilerParams(vmem_limit_bytes=2 << 20),
        name="add",
    )(*in_vmem(*arrays))


def update_kernel(part_ref, own_ref, out_ref, *, points, comps):
    s = jnp.sum(part_ref[...], axis=0)
    d = s.shape[1]
    first = s[:ROWS]
    second = s[ROWS : 2 * ROWS]
    pair = s[2 * ROWS :]
    count = jnp.concatenate([pair[:, :1], pair[:, d // 2 : d // 2 + 1]], axis=0)
    denom = count + PRIOR
    mean = own_ref[:ROWS, :]
    var = own_ref[ROWS:, :]
    fresh = (first + PRIOR * mean) / denom
    fresh_var = (second + PRIOR * (var + mean * mean)) / denom - fresh * fresh
    logw = jnp.log((pair + PRIOR) / (points + PRIOR * comps))
    for i in range(out_ref.shape[0]):
        out_ref[i, :ROWS, :] = fresh
        out_ref[i, ROWS : 2 * ROWS, :] = fresh_var
        out_ref[i, 2 * ROWS :, :] = logw


def unpack_kernel(at_ref, *refs):
    *parts, mean_ref, var_ref, logw_ref = refs
    d = mean_ref.shape[1]
    rows = mean_ref.shape[0] // len(parts)
    for i, ref in enumerate(parts):
        at = pl.ds(pl.multiple_of((at_ref[0] if i == 0 else 1 - at_ref[0]) * rows, rows), rows)
        mean_ref[at, :] = ref[:, :ROWS, :].reshape(rows, d)
        var_ref[at, :] = ref[:, ROWS : 2 * ROWS, :].reshape(rows, d)
        pair = ref[:, 2 * ROWS :, :]
        both = jnp.concatenate(
            [
                jnp.broadcast_to(pair[:, :, :1], pair.shape),
                jnp.broadcast_to(pair[:, :, d // 2 : d // 2 + 1], pair.shape),
            ],
            axis=1,
        ).reshape(rows, d)
        logw_ref[:, at] = jnp.swapaxes(both, 0, 1)[:1, :]


def exchanged(array, axis):
    return lax.ppermute(array, axis, [(0, 1), (1, 0)])


def per_device(points, means, variances, log_weights):
    n, d = points.shape
    k = means.shape[0]
    total_points = float(n * lax.axis_size(DP))
    total_comps = float(k * lax.axis_size(COMP))
    ring = lax.axis_size(RING)
    core = lax.axis_index("co")
    begin = core * (k // 2) + lax.axis_index(RING) * ROWS
    table = jnp.stack([1 - core, core, begin])
    e, p, q, m, local, own = densities(
        points, means, variances, log_weights, table, lax.axis_size(COMP), 2048
    )
    everyone = lax.all_to_all(local, COMP, 0, 0, tiled=True)

    def some(places, sums, first):
        return moments(table, places, e, p, q, m, sums, 4096, first)

    lik, total, other = some((0,), everyone, True)
    other = exchanged(other, "co")
    (mine,) = some((1,), total, False)
    parts = lax.all_to_all(summed(mine, other), RING, 0, 0, tiled=True)

    def update(*refs):
        update_kernel(*refs, points=total_points, comps=total_comps)

    part = pl.pallas_call(
        update, out_shape=pltpu.VMEM((ring, TALL, d), F32), name="update"
    )(*in_vmem(parts, own))
    near = lax.all_to_all(part, RING, 0, 0, tiled=True)
    fresh = [near, exchanged(near, "co")]
    smem, vmem = (pl.BlockSpec(memory_space=s) for s in (pltpu.SMEM, pltpu.VMEM))
    fresh_means, fresh_vars, fresh_logw = pl.pallas_call(
        unpack_kernel,
        in_specs=[smem] + [vmem] * 2,
        out_shape=[
            jax.ShapeDtypeStruct((k, d), F32),
            jax.ShapeDtypeStruct((k, d), F32),
            jax.ShapeDtypeStruct((1, k), F32),
        ],
        name="unpack",
    )(core.reshape(1), *in_vmem(*fresh))
    return (lik.reshape(n), fresh_means, fresh_vars, fresh_logw.reshape(k))


def solution(mesh):
    fine = Mesh(mesh.devices.reshape(8, 2, 2, 4, 2), DP + COMP)
    in_specs = (P(DP, None), P(COMP, None), P(COMP, None), P(COMP))
    out_specs = (P(DP), P(COMP, None), P(COMP, None), P(COMP))
    return jax.shard_map(
        per_device, mesh=fine, in_specs=in_specs, out_specs=out_specs, check_vma=False
    )
```

```python
import functools
import math

import jax
import jax.numpy as jnp
from jax import lax
from jax.experimental import pallas as pl
from jax.experimental.pallas import tpu as pltpu
from jax.sharding import Mesh, PartitionSpec as P

LOG_TWO_PI = math.log(2.0 * math.pi)
LOG2E = math.log2(math.e)
LN2 = math.log(2.0)
PRIOR = 1.0
LIMIT = 10
FIRST = 1024
TILE = 256
GROUPS = 16
PARTS = 4
F32 = jnp.float32
BF16 = jnp.bfloat16

DP = ("z", "xl", "co")
RING = ("xl", "z")
COMP = ("y", "xh")
ROWS = 16
TALL = 40

NT = (((1,), (1,)), ((), ()))


def halves(a):
    high = a.astype(BF16)
    low = (a - high.astype(F32)).astype(BF16)
    return high, low


def point_halves(x):
    xh, xl = halves(x)
    qh, ql = halves(x * x)
    return jnp.concatenate([xh, qh], axis=1), jnp.concatenate([xl, ql], axis=1)


def density_kernel(table_ref, x_hbm, mean_hbm, var_hbm, logw_hbm, e_ref, p_ref, q_ref, m_ref, l_ref, own_ref, w_ref, v_ref, off_ref, mean_ref, var_ref, logw_ref, x_ref, sems):
    n, d = x_ref.shape
    cuts = (0, FIRST, n)
    copies = [
        pltpu.make_async_copy(mean_hbm, mean_ref, sems.at[0]),
        pltpu.make_async_copy(var_hbm, var_ref, sems.at[1]),
        pltpu.make_async_copy(logw_hbm, logw_ref, sems.at[2]),
    ]
    chunks = [
        pltpu.make_async_copy(
            x_hbm.at[low:high, :], x_ref.at[low:high, :], sems.at[3 + i]
        )
        for i, (low, high) in enumerate(zip(cuts, cuts[1:]))
    ]
    for copy in copies + chunks:
        copy.start()
    for copy in copies:
        copy.wait()
    mean = mean_ref[...]
    var = var_ref[...]
    inverse = 1.0 / var
    scaled = mean * inverse
    size = jnp.sum(mean * scaled + jnp.log(var), axis=1, keepdims=True)
    logw = jnp.swapaxes(jnp.broadcast_to(logw_ref[...], (128, logw_ref.shape[1])), 0, 1)
    off = (logw - 0.5 * (size + d * LOG_TWO_PI)) * LOG2E
    off_ref[...] = jnp.broadcast_to(off[:, :1], off_ref.shape)
    w = jnp.concatenate([scaled * LOG2E, inverse * (-0.5 * LOG2E)], axis=1)
    w_ref[...], v_ref[...] = halves(w)
    begin = pl.multiple_of(table_ref[4], ROWS)
    own_ref[:ROWS, :] = mean_ref[pl.ds(begin, ROWS), :]
    own_ref[ROWS:, :] = var_ref[pl.ds(begin, ROWS), :]
    wh = w_ref[...]
    wl = v_ref[...]
    groups, size = GROUPS, wh.shape[0] // GROUPS

    def mul(a, b):
        return lax.dot_general(a, b, NT, preferred_element_type=F32)

    for tile in range(n // TILE):
        if tile * TILE in cuts:
            chunks[cuts.index(tile * TILE)].wait()
        rows = slice(tile * TILE, (tile + 1) * TILE)
        ph, plo = point_halves(x_ref[rows, :])
        p_ref[rows, :] = ph
        q_ref[rows, :] = plo
        logp = mul(wh, ph) + mul(wl, ph) + mul(wh, plo)
        tops = []
        sums = []
        for g in range(groups):
            at = slice(g * size, (g + 1) * size)
            part = logp[at, :] + off_ref[at, :]
            part = part.reshape(size // 8, 8, TILE)
            top = jnp.max(part, axis=0)
            e = jnp.exp2(part - top[None])
            e_ref[tile, at, :] = e.reshape(size, TILE)
            m_ref[8 * g : 8 * g + 8, rows] = top
            tops.append(top)
            sums.append(jnp.sum(e, axis=0))
        top = jnp.max(functools.reduce(jnp.maximum, tops), axis=0, keepdims=True)
        s = sum(a * jnp.exp2(t - top) for a, t in zip(sums, tops))
        local = top + jnp.log2(jnp.sum(s, axis=0, keepdims=True))
        for j in range(TILE // 128):
            row = tile * (TILE // 128) + j
            part = local[:, j * 128 : (j + 1) * 128]
            l_ref[:, row : row + 1, :] = jnp.broadcast_to(part[None], (l_ref.shape[0], 1, 128))


def densities(points, means, variances, log_weights, table, copies):
    n, d = points.shape
    k = means.shape[0]
    hbm, vmem, smem = (
        pl.BlockSpec(memory_space=s) for s in (pltpu.HBM, pltpu.VMEM, pltpu.SMEM)
    )
    return pl.pallas_call(
        density_kernel,
        in_specs=[smem] + [hbm] * 4,
        out_specs=[vmem] * 6,
        scratch_shapes=[
            pltpu.VMEM((k, 2 * d), BF16),
            pltpu.VMEM((k, 2 * d), BF16),
            pltpu.VMEM((k, TILE), F32),
            pltpu.VMEM((k, d), F32),
            pltpu.VMEM((k, d), F32),
            pltpu.VMEM((1, k), F32),
            pltpu.VMEM((n, d), F32),
            pltpu.SemaphoreType.DMA((5,)),
        ],
        out_shape=[
            pltpu.VMEM((n // TILE, k, TILE), F32),
            pltpu.VMEM((n, 2 * d), BF16),
            pltpu.VMEM((n, 2 * d), BF16),
            pltpu.VMEM((8 * GROUPS, n), F32),
            pltpu.VMEM((copies, n // 128, 128), F32),
            pltpu.VMEM((2 * ROWS, d), F32),
        ],
        compiler_params=pltpu.CompilerParams(vmem_limit_bytes=LIMIT << 20),
        cost_estimate=pl.CostEstimate(
            flops=12 * n * k * d, bytes_accessed=4 * n * (k + d), transcendentals=n * k
        ),
        name="density",
    )(
        table,
        in_hbm(points),
        in_hbm(means),
        in_hbm(variances),
        in_hbm(log_weights.reshape(1, k)),
    )


def in_hbm(array):
    return pltpu.with_memory_space_constraint(array, pltpu.HBM)


def in_vmem(*arrays):
    return [pltpu.with_memory_space_constraint(a, pltpu.VMEM) for a in arrays]


def moment_kernel(table_ref, e_ref, p_ref, q_ref, m_ref, sum_ref, *refs, block, first, places):
    if first:
        lik_hbm, total_ref, *refs = refs
        *refs, lik_ref, sem = refs
    else:
        total_ref = sum_ref
    *out_refs, acc_ref, cnt_ref = refs
    step = pl.program_id(0)
    size = e_ref.shape[1] // GROUPS
    pieces, _, d = out_refs[0].shape
    groups = pieces * ROWS // size

    @pl.when(step == 0)
    def _():
        acc_ref[...] = jnp.zeros_like(acc_ref)
        cnt_ref[...] = jnp.zeros_like(cnt_ref)
        if first:
            sums = sum_ref[...]
            top = jnp.max(sums, axis=0)
            total = top + jnp.log2(jnp.sum(jnp.exp2(sums - top[None]), axis=0))
            total_ref[...] = total
            lik_ref[...] = total * LN2
            pltpu.make_async_copy(lik_ref, lik_hbm, sem).start()

    def mul(a, b):
        return jnp.dot(a, b, preferred_element_type=F32)

    acc = None
    for tile in range(0, block, TILE):
        some = pl.ds(pl.multiple_of(step * block + tile, TILE), TILE)
        index = step * (block // TILE) + tile // TILE
        lanes = TILE // 128
        total = jnp.concatenate(
            [total_ref[pl.ds(index * lanes + j, 1), :] for j in range(lanes)], axis=1
        )
        parts = []
        for place in places:
            for g in range(groups):
                at = table_ref[place] * groups + g
                rows = pl.ds(pl.multiple_of(at * size, size), size)
                part = e_ref[index, rows, :].reshape(size // 8, 8, TILE)
                tops = m_ref[pl.ds(pl.multiple_of(at * 8, 8), 8), some]
                parts.append((part * jnp.exp2(tops - total)[None]).reshape(size, TILE))
        resp = jnp.concatenate(parts, axis=0)
        part = sum(resp[:, i : i + 128] for i in range(0, TILE, 128))
        count = part if tile == 0 else count + part
        rh, rl = halves(resp)
        ph = p_ref[some, :]
        part = mul(rh, ph) + mul(rl, ph) + mul(rh, q_ref[some, :])
        acc = part if tile == 0 else acc + part
    cnt_ref[...] += count
    acc_ref[...] += acc

    @pl.when(step == pl.num_programs(0) - 1)
    def _():
        if first:
            pltpu.make_async_copy(lik_ref, lik_hbm, sem).wait()
        count = jnp.sum(cnt_ref[...], axis=1, keepdims=True)
        count = jnp.broadcast_to(count, cnt_ref.shape).reshape(-1, pieces, 2, ROWS // 2, d)
        lane = lax.broadcasted_iota(jnp.int32, (pieces, ROWS // 2, d), 2)
        for i, out_ref in enumerate(out_refs):
            at = slice(i * pieces * ROWS, (i + 1) * pieces * ROWS)
            out_ref[:, 0:ROWS, :] = acc_ref[at, :d].reshape(pieces, ROWS, d)
            out_ref[:, ROWS : 2 * ROWS, :] = acc_ref[at, d:].reshape(pieces, ROWS, d)
            out_ref[:, 2 * ROWS :, :] = jnp.where(lane < d // 2, count[i, :, 0], count[i, :, 1])


def moments(table, places, e, p, q, m, sums, block, first):
    k = e.shape[1] // PARTS
    n, d = p.shape[0], p.shape[1] // 2
    pieces = k // ROWS
    rows = k * len(places)
    vmem = pl.BlockSpec(memory_space=pltpu.VMEM)

    def kernel(*refs):
        moment_kernel(*refs, block=block, first=first, places=places)

    out_specs = [vmem for _ in places]
    out_shape = [pltpu.VMEM((pieces, TALL, d), F32) for _ in places]
    scratch = [pltpu.VMEM((rows, 2 * d), F32), pltpu.VMEM((rows, 128), F32)]
    if first:
        out_specs = [pl.BlockSpec(memory_space=pltpu.HBM), vmem, *out_specs]
        out_shape = [pltpu.HBM((n // 128, 128), F32), pltpu.VMEM((n // 128, 128), F32), *out_shape]
        scratch += [pltpu.VMEM((n // 128, 128), F32), pltpu.SemaphoreType.DMA]
    return pl.pallas_call(
        kernel,
        grid_spec=pltpu.PrefetchScalarGridSpec(
            num_scalar_prefetch=1,
            grid=(n // block,),
            in_specs=[vmem] * 5,
            out_specs=out_specs,
            scratch_shapes=scratch,
        ),
        out_shape=out_shape,
        compiler_params=pltpu.CompilerParams(vmem_limit_bytes=LIMIT << 20),
        cost_estimate=pl.CostEstimate(
            flops=12 * n * rows * d, bytes_accessed=4 * n * (rows + d), transcendentals=n
        ),
        name="moment",
    )(table, *in_vmem(e, p, q, m, sums))


def summed(*arrays):
    def kernel(*refs):
        refs[-1][...] = functools.reduce(lambda a, b: a + b, [r[...] for r in refs[:-1]])

    return pl.pallas_call(
        kernel,
        out_shape=pltpu.VMEM(arrays[0].shape, F32),
        compiler_params=pltpu.CompilerParams(vmem_limit_bytes=2 << 20),
        name="add",
    )(*in_vmem(*arrays))


def update_kernel(part_ref, own_ref, out_ref, *, points, comps):
    s = jnp.sum(part_ref[...], axis=0)
    d = s.shape[1]
    first = s[:ROWS]
    second = s[ROWS : 2 * ROWS]
    pair = s[2 * ROWS :]
    count = jnp.concatenate([pair[:, :1], pair[:, d // 2 : d // 2 + 1]], axis=0)
    denom = count + PRIOR
    mean = own_ref[:ROWS, :]
    var = own_ref[ROWS:, :]
    fresh = (first + PRIOR * mean) / denom
    fresh_var = (second + PRIOR * (var + mean * mean)) / denom - fresh * fresh
    logw = jnp.log((pair + PRIOR) / (points + PRIOR * comps))
    for i in range(out_ref.shape[0]):
        out_ref[i, :ROWS, :] = fresh
        out_ref[i, ROWS : 2 * ROWS, :] = fresh_var
        out_ref[i, 2 * ROWS :, :] = logw


def unpack_kernel(at_ref, *refs):
    *parts, mean_ref, var_ref, logw_ref = refs
    d = mean_ref.shape[1]
    rows = mean_ref.shape[0] // len(parts)
    for i, ref in enumerate(parts):
        at = pl.ds(pl.multiple_of((at_ref[0] if i == 0 else 1 - at_ref[0]) * rows, rows), rows)
        mean_ref[at, :] = ref[:, :ROWS, :].reshape(rows, d)
        var_ref[at, :] = ref[:, ROWS : 2 * ROWS, :].reshape(rows, d)
        pair = ref[:, 2 * ROWS :, :]
        both = jnp.concatenate(
            [
                jnp.broadcast_to(pair[:, :, :1], pair.shape),
                jnp.broadcast_to(pair[:, :, d // 2 : d // 2 + 1], pair.shape),
            ],
            axis=1,
        ).reshape(rows, d)
        logw_ref[:, at] = jnp.swapaxes(both, 0, 1)[:1, :]


def exchanged(array, axis):
    return lax.ppermute(array, axis, [(0, 1), (1, 0)])


def per_device(points, means, variances, log_weights):
    n, d = points.shape
    k = means.shape[0]
    total_points = float(n * lax.axis_size(DP))
    total_comps = float(k * lax.axis_size(COMP))
    ring = lax.axis_size(RING)
    core = lax.axis_index("co")
    side = lax.axis_index("xl")
    begin = (core * 2 + side) * (k // 4) + lax.axis_index("z") * ROWS
    far = 1 - core
    table = jnp.stack([far * 2 + 1 - side, core * 2 + 1 - side, far * 2 + side, core * 2 + side, begin])
    e, p, q, m, local, own = densities(
        points, means, variances, log_weights, table, lax.axis_size(COMP)
    )
    everyone = lax.all_to_all(local, COMP, 0, 0, tiled=True)

    def some(places, sums, first=False):
        return moments(table, places, e, p, q, m, sums, n, first)

    lik, total, away = some((0,), everyone, True)
    away = exchanged(away, "co")
    (near,) = some((1,), total)
    away, total = lax.optimization_barrier((summed(near, away), total))
    away = exchanged(away, "xl")
    (other,) = some((2,), total)
    other = exchanged(other, "co")
    (mine,) = some((3,), total)
    parts = lax.all_to_all(summed(mine, other, away), "z", 0, 0, tiled=True)

    def update(*refs):
        update_kernel(*refs, points=total_points, comps=total_comps)

    part = pl.pallas_call(
        update, out_shape=pltpu.VMEM((ring, TALL, d), F32), name="update"
    )(*in_vmem(parts, own))
    near = lax.all_to_all(part, RING, 0, 0, tiled=True)
    fresh = [near, exchanged(near, "co")]
    smem, vmem = (pl.BlockSpec(memory_space=s) for s in (pltpu.SMEM, pltpu.VMEM))
    fresh_means, fresh_vars, fresh_logw = pl.pallas_call(
        unpack_kernel,
        in_specs=[smem] + [vmem] * 2,
        out_shape=[
            jax.ShapeDtypeStruct((k, d), F32),
            jax.ShapeDtypeStruct((k, d), F32),
            jax.ShapeDtypeStruct((1, k), F32),
        ],
        name="unpack",
    )(core.reshape(1), *in_vmem(*fresh))
    return (lik.reshape(n), fresh_means, fresh_vars, fresh_logw.reshape(k))


def solution(mesh):
    fine = Mesh(mesh.devices.reshape(8, 2, 2, 4, 2), DP + COMP)
    in_specs = (P(DP, None), P(COMP, None), P(COMP, None), P(COMP))
    out_specs = (P(DP), P(COMP, None), P(COMP, None), P(COMP))
    return jax.shard_map(
        per_device, mesh=fine, in_specs=in_specs, out_specs=out_specs, check_vma=False
    )
```

```python
import functools
import math

import jax
import jax.numpy as jnp
from jax import lax
from jax.experimental import pallas as pl
from jax.experimental.pallas import tpu as pltpu
from jax.sharding import Mesh, PartitionSpec as P

LOG_TWO_PI = math.log(2.0 * math.pi)
LOG2E = math.log2(math.e)
LN2 = math.log(2.0)
PRIOR = 1.0
LIMIT = 10
FIRST = 1024
TILE = 256
GROUPS = 16
PARTS = 4
F32 = jnp.float32
BF16 = jnp.bfloat16

DP = ("z", "xl", "co")
RING = ("xl", "z")
COMP = ("y", "xh")
ROWS = 16
TALL = 40

NT = (((1,), (1,)), ((), ()))


def halves(a):
    high = a.astype(BF16)
    low = (a - high.astype(F32)).astype(BF16)
    return high, low


def point_halves(x):
    xh, xl = halves(x)
    qh, ql = halves(x * x)
    return jnp.concatenate([xh, qh], axis=1), jnp.concatenate([xl, ql], axis=1)


def density_kernel(table_ref, x_hbm, mean_hbm, var_hbm, logw_hbm, e_ref, p_ref, q_ref, m_ref, l_ref, own_ref, w_ref, v_ref, off_ref, mean_ref, var_ref, logw_ref, x_ref, sems):
    n, d = x_ref.shape
    cuts = (0, FIRST, n)
    copies = [
        pltpu.make_async_copy(mean_hbm, mean_ref, sems.at[0]),
        pltpu.make_async_copy(var_hbm, var_ref, sems.at[1]),
        pltpu.make_async_copy(logw_hbm, logw_ref, sems.at[2]),
    ]
    chunks = [
        pltpu.make_async_copy(
            x_hbm.at[low:high, :], x_ref.at[low:high, :], sems.at[3 + i]
        )
        for i, (low, high) in enumerate(zip(cuts, cuts[1:]))
    ]
    for copy in copies + chunks:
        copy.start()
    for copy in copies:
        copy.wait()
    mean = mean_ref[...]
    var = var_ref[...]
    inverse = 1.0 / var
    scaled = mean * inverse
    size = jnp.sum(mean * scaled + jnp.log(var), axis=1, keepdims=True)
    logw = jnp.swapaxes(jnp.broadcast_to(logw_ref[...], (128, logw_ref.shape[1])), 0, 1)
    off = (logw - 0.5 * (size + d * LOG_TWO_PI)) * LOG2E
    off_ref[...] = jnp.broadcast_to(off[:, :1], off_ref.shape)
    w = jnp.concatenate([scaled * LOG2E, inverse * (-0.5 * LOG2E)], axis=1)
    w_ref[...], v_ref[...] = halves(w)
    begin = pl.multiple_of(table_ref[4], ROWS)
    own_ref[:ROWS, :] = mean_ref[pl.ds(begin, ROWS), :]
    own_ref[ROWS:, :] = var_ref[pl.ds(begin, ROWS), :]
    wh = w_ref[...]
    wl = v_ref[...]
    groups, size = GROUPS, wh.shape[0] // GROUPS

    def mul(a, b):
        return lax.dot_general(a, b, NT, preferred_element_type=F32)

    for tile in range(n // TILE):
        if tile * TILE in cuts:
            chunks[cuts.index(tile * TILE)].wait()
        rows = slice(tile * TILE, (tile + 1) * TILE)
        ph, plo = point_halves(x_ref[rows, :])
        p_ref[rows, :] = ph
        q_ref[rows, :] = plo
        logp = mul(wh, ph) + mul(wl, ph) + mul(wh, plo)
        tops = []
        sums = []
        for g in range(groups):
            at = slice(g * size, (g + 1) * size)
            part = logp[at, :] + off_ref[at, :]
            part = part.reshape(size // 8, 8, TILE)
            top = jnp.max(part, axis=0)
            e = jnp.exp2(part - top[None])
            e_ref[tile, at, :] = e.reshape(size, TILE)
            m_ref[8 * g : 8 * g + 8, rows] = top
            tops.append(top)
            sums.append(jnp.sum(e, axis=0))
        top = jnp.max(functools.reduce(jnp.maximum, tops), axis=0, keepdims=True)
        s = sum(a * jnp.exp2(t - top) for a, t in zip(sums, tops))
        local = top + jnp.log2(jnp.sum(s, axis=0, keepdims=True))
        for j in range(TILE // 128):
            row = tile * (TILE // 128) + j
            part = local[:, j * 128 : (j + 1) * 128]
            l_ref[:, row : row + 1, :] = jnp.broadcast_to(part[None], (l_ref.shape[0], 1, 128))


def densities(points, means, variances, log_weights, table, copies):
    n, d = points.shape
    k = means.shape[0]
    hbm, vmem, smem = (
        pl.BlockSpec(memory_space=s) for s in (pltpu.HBM, pltpu.VMEM, pltpu.SMEM)
    )
    return pl.pallas_call(
        density_kernel,
        in_specs=[smem] + [hbm] * 4,
        out_specs=[vmem] * 6,
        scratch_shapes=[
            pltpu.VMEM((k, 2 * d), BF16),
            pltpu.VMEM((k, 2 * d), BF16),
            pltpu.VMEM((k, TILE), F32),
            pltpu.VMEM((k, d), F32),
            pltpu.VMEM((k, d), F32),
            pltpu.VMEM((1, k), F32),
            pltpu.VMEM((n, d), F32),
            pltpu.SemaphoreType.DMA((5,)),
        ],
        out_shape=[
            pltpu.VMEM((n // TILE, k, TILE), F32),
            pltpu.VMEM((n, 2 * d), BF16),
            pltpu.VMEM((n, 2 * d), BF16),
            pltpu.VMEM((8 * GROUPS, n), F32),
            pltpu.VMEM((copies, n // 128, 128), F32),
            pltpu.VMEM((2 * ROWS, d), F32),
        ],
        compiler_params=pltpu.CompilerParams(vmem_limit_bytes=LIMIT << 20),
        cost_estimate=pl.CostEstimate(
            flops=12 * n * k * d, bytes_accessed=4 * n * (k + d), transcendentals=n * k
        ),
        name="density",
    )(
        table,
        in_hbm(points),
        in_hbm(means),
        in_hbm(variances),
        in_hbm(log_weights.reshape(1, k)),
    )


def in_hbm(array):
    return pltpu.with_memory_space_constraint(array, pltpu.HBM)


def in_vmem(*arrays):
    return [pltpu.with_memory_space_constraint(a, pltpu.VMEM) for a in arrays]


def moment_kernel(table_ref, e_ref, p_ref, q_ref, m_ref, sum_ref, *refs, block, first, places):
    if first:
        lik_ref, total_ref, *refs = refs
    else:
        total_ref = sum_ref
    *out_refs, acc_ref, cnt_ref = refs
    step = pl.program_id(0)
    size = e_ref.shape[1] // GROUPS
    pieces, _, d = out_refs[0].shape
    groups = pieces * ROWS // size

    @pl.when(step == 0)
    def _():
        acc_ref[...] = jnp.zeros_like(acc_ref)
        cnt_ref[...] = jnp.zeros_like(cnt_ref)
        if first:
            sums = sum_ref[...]
            top = jnp.max(sums, axis=0)
            total = top + jnp.log2(jnp.sum(jnp.exp2(sums - top[None]), axis=0))
            total_ref[...] = total
            lik_ref[...] = total * LN2

    def mul(a, b):
        return jnp.dot(a, b, preferred_element_type=F32)

    acc = None
    for tile in range(0, block, TILE):
        some = pl.ds(pl.multiple_of(step * block + tile, TILE), TILE)
        index = step * (block // TILE) + tile // TILE
        lanes = TILE // 128
        total = jnp.concatenate(
            [total_ref[pl.ds(index * lanes + j, 1), :] for j in range(lanes)], axis=1
        )
        parts = []
        for place in places:
            for g in range(groups):
                at = table_ref[place] * groups + g
                rows = pl.ds(pl.multiple_of(at * size, size), size)
                part = e_ref[index, rows, :].reshape(size // 8, 8, TILE)
                tops = m_ref[pl.ds(pl.multiple_of(at * 8, 8), 8), some]
                parts.append((part * jnp.exp2(tops - total)[None]).reshape(size, TILE))
        resp = jnp.concatenate(parts, axis=0)
        part = sum(resp[:, i : i + 128] for i in range(0, TILE, 128))
        count = part if tile == 0 else count + part
        rh, rl = halves(resp)
        ph = p_ref[some, :]
        part = mul(rh, ph) + mul(rl, ph) + mul(rh, q_ref[some, :])
        acc = part if tile == 0 else acc + part
    cnt_ref[...] += count
    acc_ref[...] += acc

    @pl.when(step == pl.num_programs(0) - 1)
    def _():
        count = jnp.sum(cnt_ref[...], axis=1, keepdims=True)
        count = jnp.broadcast_to(count, cnt_ref.shape).reshape(-1, pieces, 2, ROWS // 2, d)
        lane = lax.broadcasted_iota(jnp.int32, (pieces, ROWS // 2, d), 2)
        for i, out_ref in enumerate(out_refs):
            at = slice(i * pieces * ROWS, (i + 1) * pieces * ROWS)
            out_ref[:, 0:ROWS, :] = acc_ref[at, :d].reshape(pieces, ROWS, d)
            out_ref[:, ROWS : 2 * ROWS, :] = acc_ref[at, d:].reshape(pieces, ROWS, d)
            out_ref[:, 2 * ROWS :, :] = jnp.where(lane < d // 2, count[i, :, 0], count[i, :, 1])


def moments(table, places, e, p, q, m, sums, block, first):
    k = e.shape[1] // PARTS
    n, d = p.shape[0], p.shape[1] // 2
    pieces = k // ROWS
    rows = k * len(places)
    vmem = pl.BlockSpec(memory_space=pltpu.VMEM)

    def kernel(*refs):
        moment_kernel(*refs, block=block, first=first, places=places)

    out_specs = [vmem for _ in places]
    out_shape = [pltpu.VMEM((pieces, TALL, d), F32) for _ in places]
    scratch = [pltpu.VMEM((rows, 2 * d), F32), pltpu.VMEM((rows, 128), F32)]
    if first:
        out_specs = [vmem, vmem, *out_specs]
        out_shape = [pltpu.VMEM((n // 128, 128), F32)] * 2 + out_shape
    return pl.pallas_call(
        kernel,
        grid_spec=pltpu.PrefetchScalarGridSpec(
            num_scalar_prefetch=1,
            grid=(n // block,),
            in_specs=[vmem] * 5,
            out_specs=out_specs,
            scratch_shapes=scratch,
        ),
        out_shape=out_shape,
        compiler_params=pltpu.CompilerParams(vmem_limit_bytes=LIMIT << 20),
        cost_estimate=pl.CostEstimate(
            flops=12 * n * rows * d, bytes_accessed=4 * n * (rows + d), transcendentals=n
        ),
        name="moment",
    )(table, *in_vmem(e, p, q, m, sums))


def summed(*arrays):
    def kernel(*refs):
        refs[-1][...] = functools.reduce(lambda a, b: a + b, [r[...] for r in refs[:-1]])

    return pl.pallas_call(
        kernel,
        out_shape=pltpu.VMEM(arrays[0].shape, F32),
        compiler_params=pltpu.CompilerParams(vmem_limit_bytes=2 << 20),
        name="add",
    )(*in_vmem(*arrays))


def update_kernel(part_ref, own_ref, out_ref, *, points, comps):
    s = jnp.sum(part_ref[...], axis=0)
    d = s.shape[1]
    first = s[:ROWS]
    second = s[ROWS : 2 * ROWS]
    pair = s[2 * ROWS :]
    count = jnp.concatenate([pair[:, :1], pair[:, d // 2 : d // 2 + 1]], axis=0)
    denom = count + PRIOR
    mean = own_ref[:ROWS, :]
    var = own_ref[ROWS:, :]
    fresh = (first + PRIOR * mean) / denom
    fresh_var = (second + PRIOR * (var + mean * mean)) / denom - fresh * fresh
    logw = jnp.log((pair + PRIOR) / (points + PRIOR * comps))
    for i in range(out_ref.shape[0]):
        out_ref[i, :ROWS, :] = fresh
        out_ref[i, ROWS : 2 * ROWS, :] = fresh_var
        out_ref[i, 2 * ROWS :, :] = logw


def unpack_kernel(at_ref, *refs):
    *parts, mean_ref, var_ref, logw_ref = refs
    d = mean_ref.shape[1]
    rows = mean_ref.shape[0] // len(parts)
    for i, ref in enumerate(parts):
        at = pl.ds(pl.multiple_of((at_ref[0] if i == 0 else 1 - at_ref[0]) * rows, rows), rows)
        mean_ref[at, :] = ref[:, :ROWS, :].reshape(rows, d)
        var_ref[at, :] = ref[:, ROWS : 2 * ROWS, :].reshape(rows, d)
        pair = ref[:, 2 * ROWS :, :]
        both = jnp.concatenate(
            [
                jnp.broadcast_to(pair[:, :, :1], pair.shape),
                jnp.broadcast_to(pair[:, :, d // 2 : d // 2 + 1], pair.shape),
            ],
            axis=1,
        ).reshape(rows, d)
        logw_ref[:, at] = jnp.swapaxes(both, 0, 1)[:1, :]


def exchanged(array, axis):
    return lax.ppermute(array, axis, [(0, 1), (1, 0)])


def per_device(points, means, variances, log_weights):
    n, d = points.shape
    k = means.shape[0]
    total_points = float(n * lax.axis_size(DP))
    total_comps = float(k * lax.axis_size(COMP))
    ring = lax.axis_size(RING)
    core = lax.axis_index("co")
    side = lax.axis_index("xl")
    begin = (core * 2 + side) * (k // 4) + lax.axis_index("z") * ROWS
    far = 1 - core
    table = jnp.stack([far * 2 + 1 - side, core * 2 + 1 - side, far * 2 + side, core * 2 + side, begin])
    e, p, q, m, local, own = densities(
        points, means, variances, log_weights, table, lax.axis_size(COMP)
    )
    everyone = lax.all_to_all(local, COMP, 0, 0, tiled=True)

    def some(places, sums, first=False):
        return moments(table, places, e, p, q, m, sums, n, first)

    lik, total, away = some((0,), everyone, True)
    away = exchanged(away, "co")
    (near,) = some((1,), total)
    away, total = lax.optimization_barrier((summed(near, away), total))
    away = exchanged(away, "xl")
    (other,) = some((2,), total)
    other = exchanged(other, "co")
    (mine,) = some((3,), total)
    parts = lax.all_to_all(summed(mine, other, away), "z", 0, 0, tiled=True)

    def update(*refs):
        update_kernel(*refs, points=total_points, comps=total_comps)

    part = pl.pallas_call(
        update, out_shape=pltpu.VMEM((ring, TALL, d), F32), name="update"
    )(*in_vmem(parts, own))
    near = lax.all_to_all(part, RING, 0, 0, tiled=True)
    fresh = [near, exchanged(near, "co")]
    smem, vmem = (pl.BlockSpec(memory_space=s) for s in (pltpu.SMEM, pltpu.VMEM))
    fresh_means, fresh_vars, fresh_logw = pl.pallas_call(
        unpack_kernel,
        in_specs=[smem] + [vmem] * 2,
        out_shape=[
            jax.ShapeDtypeStruct((k, d), F32),
            jax.ShapeDtypeStruct((k, d), F32),
            jax.ShapeDtypeStruct((1, k), F32),
        ],
        name="unpack",
    )(core.reshape(1), *in_vmem(*fresh))
    return (lik.reshape(n), fresh_means, fresh_vars, fresh_logw.reshape(k))


def solution(mesh):
    fine = Mesh(mesh.devices.reshape(8, 2, 2, 4, 2), DP + COMP)
    in_specs = (P(DP, None), P(COMP, None), P(COMP, None), P(COMP))
    out_specs = (P(DP), P(COMP, None), P(COMP, None), P(COMP))
    return jax.shard_map(
        per_device, mesh=fine, in_specs=in_specs, out_specs=out_specs, check_vma=False
    )
```

```python
import functools
import math

import jax
import jax.numpy as jnp
from jax import lax
from jax.experimental import pallas as pl
from jax.experimental.pallas import tpu as pltpu
from jax.sharding import Mesh, PartitionSpec as P

LOG_TWO_PI = math.log(2.0 * math.pi)
LOG2E = math.log2(math.e)
LN2 = math.log(2.0)
PRIOR = 1.0
LIMIT = 10
FIRST = 1024
TILE = 256
GROUPS = 16
PARTS = 4
F32 = jnp.float32
BF16 = jnp.bfloat16

DP = ("z", "xl", "co")
RING = ("xl", "z")
COMP = ("y", "xh")
ROWS = 16
TALL = 40

NT = (((1,), (1,)), ((), ()))


def halves(a):
    high = a.astype(BF16)
    low = (a - high.astype(F32)).astype(BF16)
    return high, low


def point_halves(x):
    xh, xl = halves(x)
    qh, ql = halves(x * x)
    return jnp.concatenate([xh, qh], axis=1), jnp.concatenate([xl, ql], axis=1)


def density_kernel(table_ref, x_hbm, mean_hbm, var_hbm, logw_hbm, e_ref, p_ref, q_ref, m_ref, l_ref, own_ref, w_ref, v_ref, off_ref, mean_ref, var_ref, logw_ref, x_ref, sems):
    n, d = x_ref.shape
    cuts = (0, FIRST, n)
    copies = [
        pltpu.make_async_copy(mean_hbm, mean_ref, sems.at[0]),
        pltpu.make_async_copy(var_hbm, var_ref, sems.at[1]),
        pltpu.make_async_copy(logw_hbm, logw_ref, sems.at[2]),
    ]
    chunks = [
        pltpu.make_async_copy(
            x_hbm.at[low:high, :], x_ref.at[low:high, :], sems.at[3 + i]
        )
        for i, (low, high) in enumerate(zip(cuts, cuts[1:]))
    ]
    for copy in copies + chunks:
        copy.start()
    for copy in copies:
        copy.wait()
    mean = mean_ref[...]
    var = var_ref[...]
    inverse = 1.0 / var
    scaled = mean * inverse
    size = jnp.sum(mean * scaled + jnp.log(var), axis=1, keepdims=True)
    logw = jnp.swapaxes(jnp.broadcast_to(logw_ref[...], (128, logw_ref.shape[1])), 0, 1)
    off = (logw - 0.5 * (size + d * LOG_TWO_PI)) * LOG2E
    off_ref[...] = jnp.broadcast_to(off[:, :1], off_ref.shape)
    w = jnp.concatenate([scaled * LOG2E, inverse * (-0.5 * LOG2E)], axis=1)
    w_ref[...], v_ref[...] = halves(w)
    begin = pl.multiple_of(table_ref[4], ROWS)
    own_ref[:ROWS, :] = mean_ref[pl.ds(begin, ROWS), :]
    own_ref[ROWS:, :] = var_ref[pl.ds(begin, ROWS), :]
    wh = w_ref[...]
    wl = v_ref[...]
    groups, size = GROUPS, wh.shape[0] // GROUPS

    def mul(a, b):
        return lax.dot_general(a, b, NT, preferred_element_type=F32)

    for tile in range(n // TILE):
        if tile * TILE in cuts:
            chunks[cuts.index(tile * TILE)].wait()
        rows = slice(tile * TILE, (tile + 1) * TILE)
        ph, plo = point_halves(x_ref[rows, :])
        p_ref[rows, :] = ph
        q_ref[rows, :] = plo
        logp = mul(wh, ph) + mul(wl, ph) + mul(wh, plo)
        tops = []
        sums = []
        for g in range(groups):
            at = slice(g * size, (g + 1) * size)
            part = logp[at, :] + off_ref[at, :]
            part = part.reshape(size // 8, 8, TILE)
            top = jnp.max(part, axis=0)
            e = jnp.exp2(part - top[None])
            e_ref[tile, at, :] = e.reshape(size, TILE)
            m_ref[8 * g : 8 * g + 8, rows] = top
            tops.append(top)
            sums.append(jnp.sum(e, axis=0))
        top = jnp.max(functools.reduce(jnp.maximum, tops), axis=0, keepdims=True)
        s = sum(a * jnp.exp2(t - top) for a, t in zip(sums, tops))
        local = top + jnp.log2(jnp.sum(s, axis=0, keepdims=True))
        for j in range(TILE // 128):
            row = tile * (TILE // 128) + j
            part = local[:, j * 128 : (j + 1) * 128]
            l_ref[:, row : row + 1, :] = jnp.broadcast_to(part[None], (l_ref.shape[0], 1, 128))


def densities(points, means, variances, log_weights, table, copies):
    n, d = points.shape
    k = means.shape[0]
    hbm, vmem, smem = (
        pl.BlockSpec(memory_space=s) for s in (pltpu.HBM, pltpu.VMEM, pltpu.SMEM)
    )
    return pl.pallas_call(
        density_kernel,
        in_specs=[smem] + [hbm] * 4,
        out_specs=[vmem] * 6,
        scratch_shapes=[
            pltpu.VMEM((k, 2 * d), BF16),
            pltpu.VMEM((k, 2 * d), BF16),
            pltpu.VMEM((k, TILE), F32),
            pltpu.VMEM((k, d), F32),
            pltpu.VMEM((k, d), F32),
            pltpu.VMEM((1, k), F32),
            pltpu.VMEM((n, d), F32),
            pltpu.SemaphoreType.DMA((5,)),
        ],
        out_shape=[
            pltpu.VMEM((n // TILE, k, TILE), F32),
            pltpu.VMEM((n, 2 * d), BF16),
            pltpu.VMEM((n, 2 * d), BF16),
            pltpu.VMEM((8 * GROUPS, n), F32),
            pltpu.VMEM((copies, n // 128, 128), F32),
            pltpu.VMEM((2 * ROWS, d), F32),
        ],
        compiler_params=pltpu.CompilerParams(vmem_limit_bytes=LIMIT << 20),
        cost_estimate=pl.CostEstimate(
            flops=12 * n * k * d, bytes_accessed=4 * n * (k + d), transcendentals=n * k
        ),
        name="density",
    )(
        table,
        in_hbm(points),
        in_hbm(means),
        in_hbm(variances),
        in_hbm(log_weights.reshape(1, k)),
    )


def in_hbm(array):
    return pltpu.with_memory_space_constraint(array, pltpu.HBM)


def in_vmem(*arrays):
    return [pltpu.with_memory_space_constraint(a, pltpu.VMEM) for a in arrays]


def moment_kernel(table_ref, e_ref, p_ref, q_ref, m_ref, sum_ref, *refs, block, first, places):
    if first:
        lik_ref, total_ref, *refs = refs
    else:
        total_ref = sum_ref
    *out_refs, acc_ref, cnt_ref = refs
    step = pl.program_id(0)
    size = e_ref.shape[1] // GROUPS
    pieces, _, d = out_refs[0].shape
    groups = pieces * ROWS // size

    if first:
        sums = sum_ref[...]
        top = jnp.max(sums, axis=0)
        total = top + jnp.log2(jnp.sum(jnp.exp2(sums - top[None]), axis=0))
        total_ref[...] = total
        lik_ref[...] = total * LN2

    def mul(a, b):
        return jnp.dot(a, b, preferred_element_type=F32)

    acc = None
    for tile in range(0, block, TILE):
        some = pl.ds(pl.multiple_of(step * block + tile, TILE), TILE)
        index = step * (block // TILE) + tile // TILE
        lanes = TILE // 128
        total = jnp.concatenate(
            [total_ref[pl.ds(index * lanes + j, 1), :] for j in range(lanes)], axis=1
        )
        parts = []
        for place in places:
            for g in range(groups):
                at = table_ref[place] * groups + g
                rows = pl.ds(pl.multiple_of(at * size, size), size)
                part = e_ref[index, rows, :].reshape(size // 8, 8, TILE)
                tops = m_ref[pl.ds(pl.multiple_of(at * 8, 8), 8), some]
                parts.append((part * jnp.exp2(tops - total)[None]).reshape(size, TILE))
        resp = jnp.concatenate(parts, axis=0)
        part = sum(resp[:, i : i + 128] for i in range(0, TILE, 128))
        count = part if tile == 0 else count + part
        rh, rl = halves(resp)
        ph = p_ref[some, :]
        part = mul(rh, ph) + mul(rl, ph) + mul(rh, q_ref[some, :])
        acc = part if tile == 0 else acc + part
    cnt_ref[...] = count
    acc_ref[...] = acc

    @pl.when(step == pl.num_programs(0) - 1)
    def _():
        count = jnp.sum(cnt_ref[...], axis=1, keepdims=True)
        count = jnp.broadcast_to(count, cnt_ref.shape).reshape(-1, pieces, 2, ROWS // 2, d)
        lane = lax.broadcasted_iota(jnp.int32, (pieces, ROWS // 2, d), 2)
        for i, out_ref in enumerate(out_refs):
            at = slice(i * pieces * ROWS, (i + 1) * pieces * ROWS)
            out_ref[:, 0:ROWS, :] = acc_ref[at, :d].reshape(pieces, ROWS, d)
            out_ref[:, ROWS : 2 * ROWS, :] = acc_ref[at, d:].reshape(pieces, ROWS, d)
            out_ref[:, 2 * ROWS :, :] = jnp.where(lane < d // 2, count[i, :, 0], count[i, :, 1])


def moments(table, places, e, p, q, m, sums, block, first):
    k = e.shape[1] // PARTS
    n, d = p.shape[0], p.shape[1] // 2
    pieces = k // ROWS
    rows = k * len(places)
    vmem = pl.BlockSpec(memory_space=pltpu.VMEM)

    def kernel(*refs):
        moment_kernel(*refs, block=block, first=first, places=places)

    out_specs = [vmem for _ in places]
    out_shape = [pltpu.VMEM((pieces, TALL, d), F32) for _ in places]
    scratch = [pltpu.VMEM((rows, 2 * d), F32), pltpu.VMEM((rows, 128), F32)]
    if first:
        out_specs = [vmem, vmem, *out_specs]
        out_shape = [pltpu.VMEM((n // 128, 128), F32)] * 2 + out_shape
    return pl.pallas_call(
        kernel,
        grid_spec=pltpu.PrefetchScalarGridSpec(
            num_scalar_prefetch=1,
            grid=(n // block,),
            in_specs=[vmem] * 5,
            out_specs=out_specs,
            scratch_shapes=scratch,
        ),
        out_shape=out_shape,
        compiler_params=pltpu.CompilerParams(vmem_limit_bytes=LIMIT << 20),
        cost_estimate=pl.CostEstimate(
            flops=12 * n * rows * d, bytes_accessed=4 * n * (rows + d), transcendentals=n
        ),
        name="moment",
    )(table, *in_vmem(e, p, q, m, sums))


def summed(*arrays):
    def kernel(*refs):
        refs[-1][...] = functools.reduce(lambda a, b: a + b, [r[...] for r in refs[:-1]])

    return pl.pallas_call(
        kernel,
        out_shape=pltpu.VMEM(arrays[0].shape, F32),
        compiler_params=pltpu.CompilerParams(vmem_limit_bytes=2 << 20),
        name="add",
    )(*in_vmem(*arrays))


def update_kernel(part_ref, own_ref, out_ref, *, points, comps):
    s = jnp.sum(part_ref[...], axis=0)
    d = s.shape[1]
    first = s[:ROWS]
    second = s[ROWS : 2 * ROWS]
    pair = s[2 * ROWS :]
    count = jnp.concatenate([pair[:, :1], pair[:, d // 2 : d // 2 + 1]], axis=0)
    denom = count + PRIOR
    mean = own_ref[:ROWS, :]
    var = own_ref[ROWS:, :]
    fresh = (first + PRIOR * mean) / denom
    fresh_var = (second + PRIOR * (var + mean * mean)) / denom - fresh * fresh
    logw = jnp.log((pair + PRIOR) / (points + PRIOR * comps))
    for i in range(out_ref.shape[0]):
        out_ref[i, :ROWS, :] = fresh
        out_ref[i, ROWS : 2 * ROWS, :] = fresh_var
        out_ref[i, 2 * ROWS :, :] = logw


def unpack_kernel(core_ref, near_ref, far_ref, mean_hbm, var_hbm, logw_hbm, row_ref, sems):
    pieces, _, d = near_ref.shape
    rows = pieces * ROWS
    halves_of = ((core_ref[0], near_ref), (1 - core_ref[0], far_ref))
    copies = []
    for i, (half, ref) in enumerate(halves_of):
        some = pl.ds(pl.multiple_of(half * pieces, pieces), pieces)
        copies += [
            pltpu.make_async_copy(ref.at[:, :ROWS, :], mean_hbm.at[some, :, :], sems.at[2 * i]),
            pltpu.make_async_copy(
                ref.at[:, ROWS : 2 * ROWS, :], var_hbm.at[some, :, :], sems.at[2 * i + 1]
            ),
        ]
    for copy in copies:
        copy.start()
    for half, ref in halves_of:
        pair = ref[:, 2 * ROWS :, :]
        both = jnp.concatenate(
            [
                jnp.broadcast_to(pair[:, :, :1], pair.shape),
                jnp.broadcast_to(pair[:, :, d // 2 : d // 2 + 1], pair.shape),
            ],
            axis=1,
        ).reshape(rows, d)
        row_ref[:, pl.ds(pl.multiple_of(half * rows, rows), rows)] = jnp.swapaxes(both, 0, 1)[:1, :]
    copies.append(pltpu.make_async_copy(row_ref, logw_hbm, sems.at[4]))
    copies[-1].start()
    for copy in copies:
        copy.wait()


def unpacked(core, near, far):
    pieces, _, d = near.shape
    smem, vmem, hbm = (pl.BlockSpec(memory_space=s) for s in (pltpu.SMEM, pltpu.VMEM, pltpu.HBM))
    return pl.pallas_call(
        unpack_kernel,
        in_specs=[smem, vmem, vmem],
        out_specs=[hbm] * 3,
        out_shape=[
            pltpu.HBM((2 * pieces, ROWS, d), F32),
            pltpu.HBM((2 * pieces, ROWS, d), F32),
            pltpu.HBM((1, 2 * pieces * ROWS), F32),
        ],
        scratch_shapes=[pltpu.VMEM((1, 2 * pieces * ROWS), F32), pltpu.SemaphoreType.DMA((5,))],
        compiler_params=pltpu.CompilerParams(vmem_limit_bytes=4 << 20),
        name="unpack",
    )(core.reshape(1), *in_vmem(near, far))


def exchanged(array, axis):
    return lax.ppermute(array, axis, [(0, 1), (1, 0)])


def per_device(points, means, variances, log_weights):
    n, d = points.shape
    k = means.shape[0]
    total_points = float(n * lax.axis_size(DP))
    total_comps = float(k * lax.axis_size(COMP))
    ring = lax.axis_size(RING)
    core = lax.axis_index("co")
    side = lax.axis_index("xl")
    begin = (core * 2 + side) * (k // 4) + lax.axis_index("z") * ROWS
    far = 1 - core
    table = jnp.stack([far * 2 + 1 - side, core * 2 + 1 - side, far * 2 + side, core * 2 + side, begin])
    e, p, q, m, local, own = densities(
        points, means, variances, log_weights, table, lax.axis_size(COMP)
    )
    everyone = lax.all_to_all(local, COMP, 0, 0, tiled=True)

    def some(places, sums, first=False):
        return moments(table, places, e, p, q, m, sums, n, first)

    lik, total, away = some((0,), everyone, True)
    away = exchanged(away, "co")
    (near,) = some((1,), total)
    away, total = lax.optimization_barrier((summed(near, away), total))
    away = exchanged(away, "xl")
    (other,) = some((2,), total)
    other = exchanged(other, "co")
    (mine,) = some((3,), total)
    parts = lax.all_to_all(summed(mine, other, away), "z", 0, 0, tiled=True)

    def update(*refs):
        update_kernel(*refs, points=total_points, comps=total_comps)

    part = pl.pallas_call(
        update, out_shape=pltpu.VMEM((ring, TALL, d), F32), name="update"
    )(*in_vmem(parts, own))
    near = lax.all_to_all(part, RING, 0, 0, tiled=True)
    far = exchanged(near, "co")
    fresh_means, fresh_vars, fresh_logw = unpacked(core, near, far)
    return (lik.reshape(n), fresh_means.reshape(k, d), fresh_vars.reshape(k, d), fresh_logw.reshape(k))


def solution(mesh):
    fine = Mesh(mesh.devices.reshape(8, 2, 2, 4, 2), DP + COMP)
    in_specs = (P(DP, None), P(COMP, None), P(COMP, None), P(COMP))
    out_specs = (P(DP), P(COMP, None), P(COMP, None), P(COMP))
    return jax.shard_map(
        per_device, mesh=fine, in_specs=in_specs, out_specs=out_specs, check_vma=False
    )
```
